256 devices in a mesh: groups: 2 (over z), seq: 128 (over x, y, core).
Axes of the slice: x: 8, y: 8, z: 2, core: 2. Of those that a mesh axis runs over, the one named last changes fastest.
The devices are a block of a 8x8x16 slice.
Arguments:
- queries: bfloat16 [16384, 4096], P(('groups', 'seq')), parts along dimension 0, may hold values from -8 to 8
- keys: bfloat16 [16384, 512], P(('groups', 'seq')), parts along dimension 0, may hold values from -8 to 8
- values: bfloat16 [16384, 512], P(('groups', 'seq')), parts along dimension 0, may hold values from -6 to 6
- block_pairs: int32 [256], P('groups'), parts along dimension 0, may hold values from 0 to 127, each once
- decode_slots: int32 [256], P('groups'), parts along dimension 0, may hold values from 0 to 127, each once
Outputs:
- attended: bfloat16 [16384, 4096], P(('groups', 'seq')), parts along dimension 0
- decode_cache: bfloat16 [256, 256, 2, 128], P(('groups', 'seq')), parts along dimension 0
The draws below stay inside these ranges and needn't reach their ends.
There are 2 independent parts, one for each index of `groups`. The reference program is written for one: setup_inputs(seed, part) draws one part's arguments, and reference() takes and returns one part's arrays. A program takes and returns all parts, laid end to end along the dimension named above; each array names one. Nothing has to cross between parts.
Inputs may be any that keep to these rules, and one draw needn't show every extreme that they name: `block_pairs`: each of 0 to 127 once. `decode_slots`: each of 0 to 127 once.
All inputs are finite; a program needn't handle non-finite values.
Results may differ from the reference program's by a relative error of at most 0.012.
The reference program's roundings to bfloat16 on the way (of `rotated_queries`, `rotated_keys` and `rounded`) count: a program that leaves them out, or rounds other values in their place, can miss the bound.
Values may be sent and summed in bfloat16 or wider, within the bound.
A program may use at most 128 MiB of HBM per device.

```python
import math
import jax
import jax.numpy as jnp
from jax import lax

HD = 128
KVH = 4
GQ = 8
TOK_DEV = 64
QH = 32
SEQ = 8192
STRIDE = 32
CACHE_LEN = 256
N_SEQ = 128


def joint_draw(key):
    query_base = jnp.clip(jax.random.normal(jax.random.fold_in(key, 101), (SEQ, QH, HD), jnp.float32), -4.0, 4.0)
    key_base = jnp.clip(jax.random.normal(jax.random.fold_in(key, 102), (SEQ, KVH, HD), jnp.float32), -4.0, 4.0)
    return (query_base, key_base)


def draw_queries(key, part):
    query_base, key_base = joint_draw(key)
    return query_base.reshape(SEQ, QH * HD).astype(jnp.bfloat16)


def draw_keys(key, part):
    query_base, key_base = joint_draw(key)
    return key_base.reshape(SEQ, KVH * HD).astype(jnp.bfloat16)


def level_of(own_key, dims, pieces, smallest, largest):
    factor_of, own = 1.0, jax.random.fold_in(own_key, 6)
    for dim, blocks in pieces:
        heights = jnp.exp(jax.random.uniform(jax.random.fold_in(own, dim), (blocks,), jnp.float32, smallest / len(pieces), largest / len(pieces)))
        factor_of = factor_of * jnp.repeat(heights, dims[dim] // blocks).reshape([-1 if axis == dim else 1 for axis in range(len(dims))])
    return factor_of


def gaussian(key, extent, deviation, reach, cuts=(), held_as=jnp.bfloat16):
    result = deviation * jax.random.normal(key, extent, jnp.float32)
    if cuts:
        result = result * level_of(key, extent, cuts, -0.22, 0.18)
    return jnp.clip(result, -reach, reach).astype(held_as)


def setup_inputs(seed: int = 0, part: int = 0) -> dict:
    arg_keys = jax.random.split(jax.random.key(seed), 6)
    own_keys = jax.random.split(jax.random.fold_in(arg_keys[5], part), 6)
    return {
        "queries": draw_queries(jax.random.fold_in(jax.random.fold_in(arg_keys[5], part), 71), part),
        "keys": draw_keys(jax.random.fold_in(jax.random.fold_in(arg_keys[5], part), 71), part),
        "values": gaussian(own_keys[2], (SEQ, KVH * HD), 1.0, 6.0, ((0, 128),)),
        "block_pairs": jax.random.permutation(own_keys[3], N_SEQ).astype(jnp.int32),
        "decode_slots": jax.random.permutation(own_keys[4], N_SEQ).astype(jnp.int32),
    }


ROPE_BASE = 500000.0
NEGATIVE = -1e+30

def rotate_rows(vectors, positions):
    half_dim = vectors.shape[-1] // 2
    frequency = ROPE_BASE ** (-(jnp.arange(half_dim, dtype=jnp.float32) * 2.0) / vectors.shape[-1])
    angles = positions.astype(jnp.float32)[:, None] * frequency[None, :]
    cosine_part = jnp.cos(angles)[:, None, :]
    sine_part = jnp.sin(angles)[:, None, :]
    first_half = vectors[..., :half_dim]
    second_half = vectors[..., half_dim:]
    return jnp.concatenate([first_half * cosine_part - second_half * sine_part, second_half * cosine_part + first_half * sine_part], axis=-1)

def token_positions(block_pairs, tok_dev):
    devices = block_pairs.shape[0]
    half_tok = tok_dev // 2
    within = jnp.arange(tok_dev, dtype=jnp.int32)
    late_flag = (within >= half_tok).astype(jnp.int32)
    block_index = block_pairs[:, None] * (1 - late_flag)[None, :] + (2 * devices - 1 - block_pairs[:, None]) * late_flag[None, :]
    return (block_index * half_tok + (within % half_tok)[None, :]).reshape(-1)

def reference(queries, keys, values, block_pairs, decode_slots):
    positions = token_positions(block_pairs, TOK_DEV)
    rotated_queries = rotate_rows(queries.astype(jnp.float32).reshape(SEQ, QH, HD), positions).astype(jnp.bfloat16)
    rotated_keys = rotate_rows(keys.astype(jnp.float32).reshape(SEQ, KVH, HD), positions).astype(jnp.bfloat16)
    value_rows = values.reshape(SEQ, KVH, HD)
    key_wide = lax.optimization_barrier(rotated_keys).astype(jnp.float32)
    value_wide = value_rows.astype(jnp.float32)
    query_wide = lax.optimization_barrier(rotated_queries).astype(jnp.float32).reshape(SEQ, KVH, GQ, HD)
    score_scale = 1.0 / math.sqrt(HD)

    def one_block(block_index):
        query_rows = lax.dynamic_slice_in_dim(query_wide, block_index * TOK_DEV, TOK_DEV, 0)
        row_pos = lax.dynamic_slice_in_dim(positions, block_index * TOK_DEV, TOK_DEV, 0)
        scores = jnp.einsum('tkgd,ukd->tkgu', query_rows, key_wide) * score_scale
        allowed = (positions[None, :] <= row_pos[:, None])[:, None, None, :]
        maxima = lax.optimization_barrier(jnp.max(jnp.where(allowed, scores, NEGATIVE), axis=-1, keepdims=True))
        weights = jnp.where(allowed, jnp.exp(scores - maxima), 0.0)
        totals = lax.optimization_barrier(jnp.sum(weights, axis=-1))
        rounded = lax.optimization_barrier(weights.astype(jnp.bfloat16)).astype(jnp.float32)
        mixture = jnp.einsum('tkgu,ukd->tkgd', rounded, value_wide)
        return (mixture / totals[..., None]).astype(jnp.bfloat16).reshape(TOK_DEV, QH * HD)
    attended = lax.map(one_block, jnp.arange(N_SEQ, dtype=jnp.int32)).reshape(SEQ, QH * HD)
    row_of_position = jnp.zeros((SEQ,), jnp.int32).at[positions].set(jnp.arange(SEQ, dtype=jnp.int32))
    stacked = jnp.stack([rotated_keys, value_rows], axis=2)
    arranged = stacked[row_of_position].reshape(CACHE_LEN, STRIDE, KVH, 2, HD)
    picked = arranged[:, decode_slots % STRIDE, decode_slots // STRIDE]
    decode_cache = jnp.moveaxis(picked, 1, 0)
    return (attended, decode_cache)
```

```python
import functools
import math

import jax
import jax.numpy as jnp
import numpy as np
from jax import lax
from jax.experimental import pallas as pl
from jax.experimental.pallas import tpu as pltpu
from jax.sharding import PartitionSpec as P

HD = 128
KVH = 4
GQ = 8
QH = 32
ROPE_BASE = 500000.0
NEGATIVE = -1e30
MESH = pl.DeviceIdType.MESH
LOG_SCALE = math.log2(math.e) / math.sqrt(HD)
F32 = jnp.float32
BF16 = jnp.bfloat16


def place(side):
    me = lax.axis_index("seq")
    return me, me // (2 * side), (me // 2) % side, me % 2


def rotate(x, cosine, sine):
    return x * cosine + pltpu.roll(x, HD // 2, 1) * sine


def signs(h, far):
    return 1 if h in (0, far) else 2


def first_slot(h, side):
    return 0 if h == 0 else 2 * side * (2 * h - 1)


def prepare(side, pairs, slots, freq, keys, values, cosine, sine, packed, table):
    half = keys.shape[0] // 2
    devices = pairs.shape[0]
    far = side // 2
    me, x, y, core = place(side)
    own = pairs[me]
    row = lax.broadcasted_iota(jnp.int32, cosine.shape, 0)
    late = row >= half
    position = jnp.where(
        late, (2 * devices - 1 - own) * half + row - half, own * half + row
    )
    angle = position.astype(F32) * freq[...]
    lane = lax.broadcasted_iota(jnp.int32, cosine.shape, 1)
    cos_part = jnp.cos(angle)
    sin_part = jnp.sin(angle)
    sin_part = jnp.where(lane < HD // 2, -sin_part, sin_part)
    cosine[...] = cos_part
    sine[...] = sin_part
    for n in range(KVH):
        k = keys[:, n * HD : (n + 1) * HD].astype(F32)
        packed[n // 2, n % 2] = rotate(k, cos_part, sin_part).astype(BF16)
        packed[n // 2, 2 + n % 2] = values[:, n * HD : (n + 1) * HD]

    second = slots[me] // half >= KVH // 2

    def note(r, carry):
        dx = lax.rem(x - r // (2 * side) + side, side)
        dy = lax.rem(y - lax.rem(r // 2, side) + side, side)
        near = jnp.where(second, dy, dx)
        wide = jnp.where(second, dx, dy)
        i = jnp.where(
            near == 0,
            0,
            jnp.where(
                near == far,
                side - 1,
                jnp.where(near < far, 2 * near - 1, 2 * (side - near)),
            ),
        )
        back = (wide > far).astype(jnp.int32)
        h = jnp.where(wide > far, side - wide, wide)
        count = jnp.where(jnp.logical_or(h == 0, h == far), 1, 2)
        base = jnp.where(h == 0, 0, 2 * side * (2 * h - 1))
        slot = base + (lax.rem(r, 2) * count + back) * side + i
        table[pairs[r]] = slot
        return carry

    lax.fori_loop(0, devices, note, 0)


def attend(side, *refs):
    far = side // 2
    hops = far + 1
    pairs, slots, packed, queries, cosine, sine, mixture, weight, picked = refs[:9]
    rest = list(refs[9:])
    held = [[rest.pop(0) for _ in range(hops)] for _ in range(2)]
    got = [[rest.pop(0) for _ in range(hops)] for _ in range(2)]
    raw, turned, maxima, totals, found = rest[:5]
    query_sem, own_sem, near_sem, wide_sem, twin_out, twin_in = rest[5:]

    me, x, y, core = place(side)
    devices = pairs.shape[0]
    half = packed.shape[2] // 2
    rows = GQ * half
    step = 1 - 2 * core

    def chip(axis, shift):
        xs = lax.rem(x + shift + side, side) if axis == 0 else x
        ys = lax.rem(y + shift + side, side) if axis == 1 else y
        return {"seq": (xs * side + ys) * 2 + core}

    twin = {"seq": me + step}

    barrier = pltpu.get_barrier_semaphore()
    for target in (chip(0, 1), chip(0, -1), chip(1, 1), chip(1, -1), twin):
        pl.semaphore_signal(barrier, inc=1, device_id=target, device_id_type=MESH)
    load = pltpu.make_async_copy(queries, raw, query_sem)
    load.start()
    own_copies = [
        pltpu.make_async_copy(packed.at[p], held[p][0].at[core, 0], own_sem.at[p])
        for p in range(2)
    ]
    for copy in own_copies:
        copy.start()
    pl.semaphore_wait(barrier, 5)

    def remote(src, dst, send, recv, target):
        return pltpu.make_async_remote_copy(
            src_ref=src,
            dst_ref=dst,
            send_sem=send,
            recv_sem=recv,
            device_id=target,
            device_id_type=MESH,
        )

    def arrive(p, h, k):
        ref = held[p][h].at[core, k]
        remote(ref, ref, near_sem.at[p], got[p][h].at[k], twin).wait_recv()

    def near(p, src, k, target):
        remote(src, held[p][0].at[core, k], near_sem.at[p], got[p][0].at[k], target).start()

    def onward(p, h, src, k, target):
        remote(
            src, held[p][h + 1].at[core, k], wide_sem.at[p, h], got[p][h + 1].at[k], target
        ).start()

    def share(p, h, src, k):
        remote(src, held[p][h].at[core, k], twin_out.at[p, h], twin_in.at[p, h], twin).start()

    def first_tick(i):
        sources = []
        for p in range(2):
            if i == 0:
                src = packed.at[p]
                near(p, src, 1, chip(p, 1))
                near(p, src, 2, chip(p, -1))
            else:
                arrive(p, 0, i)
                src = held[p][0].at[core, i]
                k = (i + 1) // 2
                if k + 1 < far:
                    near(p, src, i + 2, chip(p, 1 if i % 2 else -1))
                elif k + 1 == far and i % 2 == 0:
                    near(p, held[p][0].at[core, i - 1 + core], side - 1, chip(p, step))
            sources.append(src)
        for p in range(2):
            onward(p, 0, sources[p], i, chip(1 - p, 1))
            onward(p, 0, sources[p], side + i, chip(1 - p, -1))
            share(p, 0, sources[p], i)

    def tick(h, i):
        for p in range(2):
            for s in range(signs(h, far)):
                k = s * side + i
                arrive(p, h, k)
                src = held[p][h].at[core, k]
                if h + 1 < far:
                    onward(p, h, src, k, chip(1 - p, 1 - 2 * s))
            if h + 1 == far:
                onward(p, h, held[p][h].at[core, core * side + i], i, chip(1 - p, step))
            for s in range(signs(h, far)):
                share(p, h, held[p][h].at[core, s * side + i], s * side + i)

    def turn(n):
        for g in range(GQ):
            q = n * GQ + g
            r = rotate(raw[:, q * HD : (q + 1) * HD].astype(F32), cosine[...], sine[...])
            r = r.astype(BF16)
            turned[n, g * half : (g + 1) * half] = r[:half]
            turned[n, rows + g * half : rows + (g + 1) * half] = r[half:]

    def scores(key_rows, query_rows):
        return lax.dot_general(
            key_rows, query_rows, (((1,), (1,)), ((), ())), preferred_element_type=F32
        )

    def mix(value_rows, weights):
        return lax.dot_general(
            value_rows, weights, (((0,), (0,)), ((), ())), preferred_element_type=F32
        )

    def begin(n):
        p, hh = n // 2, n % 2
        keys, values = packed[p, hh], packed[p, 2 + hh]
        u = lax.broadcasted_iota(jnp.int32, (half, rows), 0)
        t = lax.rem(lax.broadcasted_iota(jnp.int32, (half, rows), 1), half)
        for z in range(2):
            span = pl.ds(z * rows, rows)
            part = slice(z * half, (z + 1) * half)
            s = scores(keys[part], turned[n, span])
            s = jnp.where(u <= t, s, NEGATIVE)
            top = jnp.max(s, axis=0, keepdims=True)
            w = jnp.exp2((s - top) * LOG_SCALE)
            maxima[n, :, span] = top
            totals[n, :, span] = jnp.sum(w.reshape(half // 8, 8, rows), axis=0)
            mixture[n, :, span] = mix(values[part], w.astype(BF16))

    own = pairs[me]

    def block_of(p, h, cc, s, i):
        dx = 0 if i == 0 else far if i == side - 1 else (i + 1) // 2 if i % 2 else -(i // 2)
        shift = (1 - 2 * s) * h
        a = lax.rem((x if p == 0 else y) - dx + side, side)
        b = lax.rem((y if p == 0 else x) - shift + side, side)
        xs, ys = (a, b) if p == 0 else (b, a)
        return pairs[(xs * side + ys) * 2 + cc]

    def unit(p, h, cc, s, hh, early_bias, late_bias):
        n = 2 * p + hh
        ref = held[p][h]
        span = pl.ds(pl.multiple_of(s * side, side), side)
        count = side * half
        query_rows = turned[n]
        early = ref[cc, span, hh, :half].reshape(count, HD)
        late = ref[cc, span, hh, half:].reshape(count, HD)
        es = scores(early, query_rows)
        ls = scores(late, query_rows[rows:])
        e_parts = [
            es[i * half : (i + 1) * half, :rows] + early_bias[i] for i in range(side)
        ]
        f_part = es[:, rows:]
        l_parts = [ls[i * half : (i + 1) * half] + late_bias[i] for i in range(side)]
        e_top = functools.reduce(jnp.maximum, e_parts)
        l_top = functools.reduce(jnp.maximum, l_parts)
        f_top = jnp.max(f_part.reshape(side, half, rows), axis=0)
        top = jnp.concatenate([e_top, jnp.maximum(l_top, f_top)], axis=1)
        old = maxima[n]
        top = jnp.maximum(jnp.max(top, axis=0, keepdims=True), old)
        factor = jnp.exp2((old - top) * LOG_SCALE)
        maxima[n] = top
        level = top * LOG_SCALE
        e_level, l_level = level[:, :rows], level[:, rows:]
        ew = [jnp.exp2(v * LOG_SCALE - e_level) for v in e_parts]
        lw = [jnp.exp2(v * LOG_SCALE - l_level) for v in l_parts]
        fw = jnp.exp2(f_part * LOG_SCALE - l_level)
        e_sum = functools.reduce(jnp.add, ew).reshape(half // 8, 8, rows).sum(axis=0)
        l_sum = functools.reduce(jnp.add, lw).reshape(half // 8, 8, rows).sum(axis=0)
        f_sum = fw.reshape(count // 8, 8, rows).sum(axis=0)
        totals[n] = totals[n] * factor + jnp.concatenate([e_sum, l_sum + f_sum], axis=1)
        early_values = ref[cc, span, 2 + hh, :half].reshape(count, HD)
        late_values = ref[cc, span, 2 + hh, half:].reshape(count, HD)
        ew = jnp.concatenate([v.astype(BF16) for v in ew], axis=0)
        lw = jnp.concatenate([v.astype(BF16) for v in lw], axis=0)
        mixture[n, :, :rows] = mixture[n, :, :rows] * factor[:, :rows] + mix(early_values, ew)
        mixture[n, :, rows:] = (
            mixture[n, :, rows:] * factor[:, rows:]
            + mix(early_values, fw.astype(BF16))
            + mix(late_values, lw)
        )

    wanted = slots[me]
    wanted_head = wanted // half
    tile = lax.broadcasted_iota(jnp.int32, (16, HD), 0)
    picks = [
        [
            jnp.where(
                jnp.logical_and(
                    tile + part * 16 == lax.rem(wanted, half), lax.rem(wanted_head, 2) == hh
                ),
                1.0,
                0.0,
            ).astype(BF16)
            for part in range(half // 16)
        ]
        for hh in range(2)
    ]

    def collect(p, h, g, cc, s):
        span = pl.ds(pl.multiple_of(s * side, side), side)
        slot = pl.multiple_of(first_slot(h, side) + g * side, side)
        for z in range(2):
            for kind in range(2):
                terms = [
                    held[p][h][
                        cc, span, 2 * kind + hh, z * half + part * 16 : z * half + part * 16 + 16
                    ]
                    * picks[hh][part][None]
                    for hh in range(2)
                    for part in range(half // 16)
                ]
                row = functools.reduce(jnp.add, terms).astype(F32)
                found[p, 2 * z + kind, pl.ds(slot, side)] = jnp.sum(row, axis=1)

    def process(h, g):
        cc, s = g // signs(h, far), lax.rem(g, signs(h, far))
        for p in range(2):
            blocks = [block_of(p, h, cc, s, i) for i in range(side)]
            early_bias = [jnp.where(b < own, 0.0, NEGATIVE) for b in blocks]
            late_bias = [jnp.where(b > own, 0.0, NEGATIVE) for b in blocks]
            for hh in range(2):
                unit(p, h, cc, s, hh, early_bias, late_bias)
            collect(p, h, g, cc, s)

    def from_twin(h):
        for p in range(2):
            ref = held[p][h].at[1 - core]
            remote(ref, ref, twin_out.at[p, h], twin_in.at[p, h], twin).wait_recv()

    for i in range(side):
        first_tick(i)
        if i == 0:
            load.wait()
        if i < KVH:
            turn(i)
            begin(i)
    for copy in own_copies:
        copy.wait()

    for h in range(1, hops):
        groups = 2 * signs(h - 1, far)
        ticks = side // groups

        def ticks_of(g, h=h, ticks=ticks):
            for k in range(ticks):
                tick(h, g * ticks + k)

        ticks_of(0)
        from_twin(h - 1)

        def body(g, carry, h=h, groups=groups, ticks_of=ticks_of):
            process(h - 1, g)

            @pl.when(g + 1 < groups)
            def _():
                ticks_of(g + 1)

            return carry

        lax.fori_loop(0, groups, body, 0)

    from_twin(far)

    def last(g, carry):
        process(far, g)
        return carry

    lax.fori_loop(0, 2, last, 0)

    weight[...] = totals[...]
    second = wanted_head >= KVH // 2
    for kind in range(4):
        picked[kind] = jnp.where(second, found[1, kind], found[0, kind])

    for p in range(2):
        ref = held[p][0].at[core, pl.ds(1, side - 1)]
        remote(ref, ref, near_sem.at[p], got[p][0].at[0], twin).wait_send()
        for h in range(hops):
            if h < far:
                ref = held[p][h + 1].at[core]
                remote(ref, ref, wide_sem.at[p, h], got[p][0].at[0], twin).wait_send()
            ref = held[p][h].at[core]
            remote(ref, ref, twin_out.at[p, h], twin_in.at[p, h], twin).wait_send()


def finish(table, mixture, weight, picked, out, cache):
    half = out.shape[0] // 2
    rows = GQ * half
    devices = table.shape[0]
    for n in range(KVH):
        total = jnp.sum(weight[n], axis=0, keepdims=True)
        done = jnp.transpose(mixture[n] * (1.0 / total)).astype(BF16)
        for z in range(2):
            for g in range(GQ):
                q = n * GQ + g
                out[z * half : (z + 1) * half, q * HD : (q + 1) * HD] = done[
                    z * rows + g * half : z * rows + (g + 1) * half
                ]

    def emit(j, carry):
        slot = table[j]
        for z in range(2):
            pair = [picked[2 * z + kind, pl.ds(slot, 1)] for kind in range(2)]
            where = j if z == 0 else 2 * devices - 1 - j
            cache[where] = jnp.concatenate(pair, axis=0).astype(BF16)
        return carry

    lax.fori_loop(0, devices, emit, 0, unroll=4)


def shards(side, queries, keys, values, block_pairs, decode_slots):
    tok_dev = queries.shape[0]
    devices = block_pairs.shape[0]
    half = tok_dev // 2
    far = side // 2
    rows = GQ * half
    whole = 2 * rows
    exponent = -2.0 * (np.arange(HD) % (HD // 2)) / HD
    freq = jnp.asarray((ROPE_BASE**exponent).astype(np.float32)[None, :])
    vmem = pl.BlockSpec(memory_space=pltpu.VMEM)
    smem = pl.BlockSpec(memory_space=pltpu.SMEM)
    cosine, sine, packed, table = pl.pallas_call(
        functools.partial(prepare, side),
        out_shape=(
            jax.ShapeDtypeStruct((tok_dev, HD), F32),
            jax.ShapeDtypeStruct((tok_dev, HD), F32),
            jax.ShapeDtypeStruct((2, 4, tok_dev, HD), BF16),
            jax.ShapeDtypeStruct((devices,), jnp.int32),
        ),
        in_specs=[smem, smem, vmem, vmem, vmem],
        out_specs=(vmem, vmem, vmem, smem),
    )(block_pairs, decode_slots, freq, keys, values)
    held = [
        pltpu.VMEM((2, signs(h, far) * side, 4, tok_dev, HD), BF16) for h in range(far + 1)
    ]
    got = [pltpu.SemaphoreType.DMA((signs(h, far) * side,)) for h in range(far + 1)]
    mixture, weight, picked = pl.pallas_call(
        functools.partial(attend, side),
        out_shape=(
            jax.ShapeDtypeStruct((KVH, HD, whole), F32),
            jax.ShapeDtypeStruct((KVH, 8, whole), F32),
            jax.ShapeDtypeStruct((4, devices, HD), F32),
        ),
        in_specs=[smem, smem, vmem, pl.BlockSpec(memory_space=pl.ANY), vmem, vmem],
        out_specs=(vmem, vmem, vmem),
        scratch_shapes=[
            *held,
            *held,
            *got,
            *got,
            pltpu.VMEM((tok_dev, QH * HD), BF16),
            pltpu.VMEM((KVH, whole, HD), BF16),
            pltpu.VMEM((KVH, 1, whole), F32),
            pltpu.VMEM((KVH, 8, whole), F32),
            pltpu.VMEM((2, 4, devices, HD), F32),
            pltpu.SemaphoreType.DMA,
            pltpu.SemaphoreType.DMA((2,)),
            pltpu.SemaphoreType.DMA((2,)),
            pltpu.SemaphoreType.DMA((2, far)),
            pltpu.SemaphoreType.DMA((2, far + 1)),
            pltpu.SemaphoreType.DMA((2, far + 1)),
        ],
        compiler_params=pltpu.CompilerParams(
            collective_id=0, has_side_effects=True, vmem_limit_bytes=60 * 1024 * 1024
        ),
    )(block_pairs, decode_slots, packed, queries, cosine, sine)
    attended, cache = pl.pallas_call(
        finish,
        out_shape=(
            jax.ShapeDtypeStruct((tok_dev, QH * HD), BF16),
            jax.ShapeDtypeStruct((2 * devices, 2, HD), BF16),
        ),
        in_specs=[smem, vmem, vmem, vmem],
        out_specs=(vmem, vmem),
    )(table, mixture, weight, picked)
    return attended, cache[None]


def solution(mesh):
    side = math.isqrt(mesh.shape["seq"] // 2)
    placed = (
        P(("groups", "seq"), None),
        P(("groups", "seq"), None),
        P(("groups", "seq"), None),
        P("groups"),
        P("groups"),
    )
    return jax.shard_map(
        functools.partial(shards, side),
        mesh=mesh,
        in_specs=placed,
        out_specs=(P(("groups", "seq"), None), P(("groups", "seq"), None, None, None)),
        check_vma=False,
    )
```

```python
import functools
import math

import jax
import jax.numpy as jnp
import numpy as np
from jax import lax
from jax.experimental import pallas as pl
from jax.experimental.pallas import tpu as pltpu
from jax.sharding import PartitionSpec as P

HD = 128
KVH = 4
GQ = 8
QH = 32
ROPE_BASE = 500000.0
NEGATIVE = -1e30
MESH = pl.DeviceIdType.MESH
LOG_SCALE = math.log2(math.e) / math.sqrt(HD)
F32 = jnp.float32
BF16 = jnp.bfloat16


def place(side):
    me = lax.axis_index("seq")
    return me, me // (2 * side), (me // 2) % side, me % 2


def rotate(x, cosine, sine):
    return x * cosine + pltpu.roll(x, HD // 2, 1) * sine


def signs(h, far):
    return 1 if h in (0, far) else 2


def first_slot(h, side):
    return 0 if h == 0 else 2 * side * (2 * h - 1)


def prepare(side, pairs, freq, keys, values, cosine, sine, packed):
    half = keys.shape[0] // 2
    devices = pairs.shape[0]
    own = pairs[place(side)[0]]
    row = lax.broadcasted_iota(jnp.int32, cosine.shape, 0)
    late = row >= half
    position = jnp.where(
        late, (2 * devices - 1 - own) * half + row - half, own * half + row
    )
    angle = position.astype(F32) * freq[...]
    lane = lax.broadcasted_iota(jnp.int32, cosine.shape, 1)
    cos_part = jnp.cos(angle)
    sin_part = jnp.sin(angle)
    sin_part = jnp.where(lane < HD // 2, -sin_part, sin_part)
    cosine[...] = cos_part
    sine[...] = sin_part
    for n in range(KVH):
        k = keys[:, n * HD : (n + 1) * HD].astype(F32)
        packed[n // 2, n % 2] = rotate(k, cos_part, sin_part).astype(BF16)
        packed[n // 2, 2 + n % 2] = values[:, n * HD : (n + 1) * HD]


def attend(side, *refs):
    far = side // 2
    hops = far + 1
    pairs, slots, packed, queries, cosine, sine, mixture, weight, picked = refs[:9]
    rest = list(refs[9:])
    held = [[rest.pop(0) for _ in range(hops)] for _ in range(2)]
    got = [[rest.pop(0) for _ in range(hops)] for _ in range(2)]
    raw, turned, maxima, totals, found = rest[:5]
    query_sem, own_sem, near_sem, wide_sem, twin_out, twin_in = rest[5:]

    me, x, y, core = place(side)
    devices = pairs.shape[0]
    half = packed.shape[2] // 2
    rows = GQ * half
    step = 1 - 2 * core

    def chip(axis, shift):
        xs = lax.rem(x + shift + side, side) if axis == 0 else x
        ys = lax.rem(y + shift + side, side) if axis == 1 else y
        return {"seq": (xs * side + ys) * 2 + core}

    twin = {"seq": me + step}

    barrier = pltpu.get_barrier_semaphore()
    for target in (chip(0, 1), chip(0, -1), chip(1, 1), chip(1, -1), twin):
        pl.semaphore_signal(barrier, inc=1, device_id=target, device_id_type=MESH)
    load = pltpu.make_async_copy(queries, raw, query_sem)
    load.start()
    own_copies = [
        pltpu.make_async_copy(packed.at[p], held[p][0].at[core, 0], own_sem.at[p])
        for p in range(2)
    ]
    for copy in own_copies:
        copy.start()
    pl.semaphore_wait(barrier, 5)

    def remote(src, dst, send, recv, target):
        return pltpu.make_async_remote_copy(
            src_ref=src,
            dst_ref=dst,
            send_sem=send,
            recv_sem=recv,
            device_id=target,
            device_id_type=MESH,
        )

    def arrive(p, h, k):
        ref = held[p][h].at[core, k]
        remote(ref, ref, near_sem.at[p], got[p][h].at[k], twin).wait_recv()

    def near(p, src, k, target):
        remote(src, held[p][0].at[core, k], near_sem.at[p], got[p][0].at[k], target).start()

    def onward(p, h, src, k, target):
        remote(
            src, held[p][h + 1].at[core, k], wide_sem.at[p, h], got[p][h + 1].at[k], target
        ).start()

    def share(p, h, src, k):
        remote(src, held[p][h].at[core, k], twin_out.at[p, h], twin_in.at[p, h], twin).start()

    def first_tick(i):
        sources = []
        for p in range(2):
            if i == 0:
                src = packed.at[p]
                near(p, src, 1, chip(p, 1))
                near(p, src, 2, chip(p, -1))
            else:
                arrive(p, 0, i)
                src = held[p][0].at[core, i]
                k = (i + 1) // 2
                if k + 1 < far:
                    near(p, src, i + 2, chip(p, 1 if i % 2 else -1))
                elif k + 1 == far and i % 2 == 0:
                    near(p, held[p][0].at[core, i - 1 + core], side - 1, chip(p, step))
            sources.append(src)
        for p in range(2):
            onward(p, 0, sources[p], i, chip(1 - p, 1))
            onward(p, 0, sources[p], side + i, chip(1 - p, -1))
            share(p, 0, sources[p], i)

    def tick(h, i):
        for p in range(2):
            for s in range(signs(h, far)):
                k = s * side + i
                arrive(p, h, k)
                src = held[p][h].at[core, k]
                if h + 1 < far:
                    onward(p, h, src, k, chip(1 - p, 1 - 2 * s))
            if h + 1 == far:
                onward(p, h, held[p][h].at[core, core * side + i], i, chip(1 - p, step))
            for s in range(signs(h, far)):
                share(p, h, held[p][h].at[core, s * side + i], s * side + i)

    def turn(n):
        for g in range(GQ):
            q = n * GQ + g
            r = rotate(raw[:, q * HD : (q + 1) * HD].astype(F32), cosine[...], sine[...])
            r = r.astype(BF16)
            for z in range(2):
                turned[n, g * half : (g + 1) * half, z * HD : (z + 1) * HD] = r[
                    z * half : (z + 1) * half
                ]

    def scores(key_rows, query_rows):
        return lax.dot_general(
            key_rows, query_rows, (((1,), (1,)), ((), ())), preferred_element_type=F32
        )

    def mix(value_rows, weights):
        return lax.dot_general(
            value_rows, weights, (((0,), (0,)), ((), ())), preferred_element_type=F32
        )

    def begin(n):
        p, hh = n // 2, n % 2
        keys, values = packed[p, hh], packed[p, 2 + hh]
        u = lax.broadcasted_iota(jnp.int32, (half, rows), 0)
        t = lax.rem(lax.broadcasted_iota(jnp.int32, (half, rows), 1), half)
        for z in range(2):
            part = slice(z * half, (z + 1) * half)
            deep = slice(z * HD, (z + 1) * HD)
            s = scores(keys[part], turned[n, :, deep])
            s = jnp.where(u <= t, s, NEGATIVE)
            top = jnp.max(s, axis=0, keepdims=True)
            w = jnp.exp2((s - top) * LOG_SCALE)
            maxima[n, z] = top
            totals[n, z] = jnp.sum(w.reshape(half // 8, 8, rows), axis=0)
            mixture[n, deep] = mix(values[part], w.astype(BF16))

    own = pairs[me]

    def block_of(p, h, cc, s, i):
        dx = 0 if i == 0 else far if i == side - 1 else (i + 1) // 2 if i % 2 else -(i // 2)
        shift = (1 - 2 * s) * h
        a = lax.rem((x if p == 0 else y) - dx + side, side)
        b = lax.rem((y if p == 0 else x) - shift + side, side)
        xs, ys = (a, b) if p == 0 else (b, a)
        return pairs[(xs * side + ys) * 2 + cc]

    def both(ref, cc, span, k, flags):
        pair = [
            ref[cc, span, k, z * half : (z + 1) * half] * flags[z] for z in range(2)
        ]
        return jnp.concatenate(pair, axis=2).reshape(side * half, 2 * HD)

    def fold(parts, op):
        return functools.reduce(op, parts)

    def tiles(v):
        return [v[8 * i : 8 * i + 8] for i in range(v.shape[0] // 8)]

    def unit_scores(p, h, cc, s, hh, flags):
        span = pl.ds(pl.multiple_of(s * side, side), side)
        ref = held[p][h]
        query_rows = turned[2 * p + hh]
        early = ref[cc, span, hh, :half].reshape(side * half, HD)
        return (
            scores(both(ref, cc, span, hh, flags), query_rows),
            scores(early, query_rows[:, HD:]),
        )

    def unit_mix(p, h, cc, s, hh, flags, early, late, pair):
        n = 2 * p + hh
        span = pl.ds(pl.multiple_of(s * side, side), side)
        ref = held[p][h]
        mixed, full = pair
        blocks = [mixed[i * half : (i + 1) * half] for i in range(side)]
        tops = [fold(tiles(v), jnp.maximum) for v in blocks]
        e_top = fold([jnp.where(early[i], tops[i], NEGATIVE) for i in range(side)], jnp.maximum)
        l_top = fold([jnp.where(late[i], tops[i], NEGATIVE) for i in range(side)], jnp.maximum)
        l_top = jnp.maximum(l_top, fold(tiles(full), jnp.maximum))
        levels, factors = [], []
        for z, top in enumerate((e_top, l_top)):
            old = maxima[n, z]
            new = jnp.maximum(jnp.max(top, axis=0, keepdims=True), old)
            factors.append(jnp.exp2((old - new) * LOG_SCALE))
            levels.append(new * LOG_SCALE)
            maxima[n, z] = new
        ws = [
            jnp.exp2(
                blocks[i] * LOG_SCALE
                - jnp.where(early[i], levels[0], jnp.where(late[i], levels[1], -NEGATIVE))
            )
            for i in range(side)
        ]
        fw = jnp.exp2(full * LOG_SCALE - levels[1])
        sums = [fold(tiles(w), jnp.add) for w in ws]
        e_sum = fold([jnp.where(early[i], sums[i], 0.0) for i in range(side)], jnp.add)
        l_sum = fold([jnp.where(late[i], sums[i], 0.0) for i in range(side)], jnp.add)
        totals[n, 0] = totals[n, 0] * factors[0] + e_sum
        totals[n, 1] = totals[n, 1] * factors[1] + (l_sum + fold(tiles(fw), jnp.add))
        w = jnp.concatenate([v.astype(BF16) for v in ws], axis=0)
        o = mix(both(ref, cc, span, 2 + hh, flags), w)
        values = ref[cc, span, 2 + hh, :half].reshape(side * half, HD)
        f = mix(values, fw.astype(BF16))
        mixture[n, :HD] = mixture[n, :HD] * factors[0] + o[:HD]
        mixture[n, HD:] = mixture[n, HD:] * factors[1] + (o[HD:] + f)

    wanted = slots[me]
    wanted_head = wanted // half
    tile = lax.broadcasted_iota(jnp.int32, (16, HD), 0)
    picks = [
        [
            jnp.where(
                jnp.logical_and(
                    tile + part * 16 == lax.rem(wanted, half), lax.rem(wanted_head, 2) == hh
                ),
                1.0,
                0.0,
            ).astype(BF16)
            for part in range(half // 16)
        ]
        for hh in range(2)
    ]

    def collect(p, h, g, cc, s):
        span = pl.ds(pl.multiple_of(s * side, side), side)
        slot = pl.multiple_of(first_slot(h, side) + g * side, side)
        for z in range(2):
            for kind in range(2):
                terms = [
                    held[p][h][
                        cc, span, 2 * kind + hh, z * half + part * 16 : z * half + part * 16 + 16
                    ]
                    * picks[hh][part][None]
                    for hh in range(2)
                    for part in range(half // 16)
                ]
                row = functools.reduce(jnp.add, terms).astype(F32)
                found[p, 2 * z + kind, pl.ds(slot, side)] = jnp.sum(row, axis=1)

    def process(h, g):
        cc, s = g // signs(h, far), lax.rem(g, signs(h, far))
        todo = []
        for p in range(2):
            blocks = [block_of(p, h, cc, s, i) for i in range(side)]
            early = [b < own for b in blocks]
            late = [b > own for b in blocks]
            flags = [
                jnp.concatenate(
                    [
                        jnp.full((1, half, HD), jnp.where(f, 1.0, 0.0), F32).astype(BF16)
                        for f in kind
                    ],
                    axis=0,
                )
                for kind in (early, late)
            ]
            for hh in range(2):
                todo.append((p, hh, flags, early, late))
        pair = unit_scores(*todo[0][:1], h, cc, s, *todo[0][1:3])
        for k, (p, hh, flags, early, late) in enumerate(todo):
            held_pair = pair
            if k + 1 < len(todo):
                pair = unit_scores(todo[k + 1][0], h, cc, s, *todo[k + 1][1:3])
            unit_mix(p, h, cc, s, hh, flags, early, late, held_pair)
        for p in range(2):
            collect(p, h, g, cc, s)

    def from_twin(h):
        for p in range(2):
            ref = held[p][h].at[1 - core]
            remote(ref, ref, twin_out.at[p, h], twin_in.at[p, h], twin).wait_recv()

    for i in range(side):
        first_tick(i)
        if i == 0:
            load.wait()
        if i < KVH:
            turn(i)
            begin(i)
    for copy in own_copies:
        copy.wait()

    for h in range(1, hops):
        groups = 2 * signs(h - 1, far)
        ticks = side // groups

        def ticks_of(g, h=h, ticks=ticks):
            for k in range(ticks):
                tick(h, g * ticks + k)

        ticks_of(0)
        from_twin(h - 1)

        def body(g, carry, h=h, groups=groups, ticks_of=ticks_of):
            process(h - 1, g)

            @pl.when(g + 1 < groups)
            def _():
                ticks_of(g + 1)

            return carry

        lax.fori_loop(0, groups, body, 0)

    from_twin(far)

    def last(g, carry):
        process(far, g)
        return carry

    lax.fori_loop(0, 2, last, 0)

    weight[...] = totals[...]
    second = wanted_head >= KVH // 2
    for kind in range(4):
        picked[kind] = jnp.where(second, found[1, kind], found[0, kind])

    for p in range(2):
        ref = held[p][0].at[core, pl.ds(1, side - 1)]
        remote(ref, ref, near_sem.at[p], got[p][0].at[0], twin).wait_send()
        for h in range(hops):
            if h < far:
                ref = held[p][h + 1].at[core]
                remote(ref, ref, wide_sem.at[p, h], got[p][0].at[0], twin).wait_send()
            ref = held[p][h].at[core]
            remote(ref, ref, twin_out.at[p, h], twin_in.at[p, h], twin).wait_send()


def finish(side, slots, pairs, mixture, weight, picked, out, cache):
    half = out.shape[0] // 2
    devices = pairs.shape[1]
    far = side // 2
    me, x, y, core = place(side)
    shape = (devices, devices)
    row = lax.broadcasted_iota(jnp.int32, shape, 0)
    r = lax.broadcasted_iota(jnp.int32, shape, 1)
    dx = lax.rem(x - r // (2 * side) + side, side)
    dy = lax.rem(y - lax.rem(r // 2, side) + side, side)
    second = slots[me] // half >= KVH // 2
    near = jnp.where(second, dy, dx)
    wide = jnp.where(second, dx, dy)
    i = jnp.where(near < far, 2 * near - 1, 2 * (side - near))
    i = jnp.where(near == far, side - 1, jnp.where(near == 0, 0, i))
    h = jnp.minimum(wide, side - wide)
    group = lax.rem(r, 2) * jnp.where(jnp.logical_or(h == 0, h == far), 1, 2)
    group = group + jnp.where(wide > far, 1, 0)
    slot = jnp.where(h == 0, 0, 2 * side * (2 * h - 1)) + group * side + i
    at_slot = jnp.where(slot == row, 1.0, 0.0).astype(BF16)
    for z in range(2):
        wanted = row if z == 0 else devices - 1 - row
        at_block = jnp.where(pairs[...] == wanted, 1.0, 0.0).astype(BF16)
        order = lax.dot_general(
            at_block, at_slot, (((1,), (1,)), ((), ())), preferred_element_type=F32
        ).astype(BF16)
        for kind in range(2):
            rows = picked[2 * z + kind].astype(BF16)
            cache[z * devices : (z + 1) * devices, kind * HD : (kind + 1) * HD] = jnp.dot(
                order, rows, preferred_element_type=F32
            ).astype(BF16)
    for n in range(KVH):
        for z in range(2):
            total = jnp.sum(weight[n, z], axis=0, keepdims=True)
            done = mixture[n, z * HD : (z + 1) * HD] * (1.0 / total)
            done = jnp.transpose(done).astype(BF16)
            for g in range(GQ):
                q = n * GQ + g
                out[z * half : (z + 1) * half, q * HD : (q + 1) * HD] = done[
                    g * half : (g + 1) * half
                ]


def shards(side, queries, keys, values, block_pairs, decode_slots):
    tok_dev = queries.shape[0]
    devices = block_pairs.shape[0]
    half = tok_dev // 2
    far = side // 2
    rows = GQ * half
    exponent = -2.0 * (np.arange(HD) % (HD // 2)) / HD
    freq = jnp.asarray((ROPE_BASE**exponent).astype(np.float32)[None, :])
    vmem = pl.BlockSpec(memory_space=pltpu.VMEM)
    smem = pl.BlockSpec(memory_space=pltpu.SMEM)
    cosine, sine, packed = pl.pallas_call(
        functools.partial(prepare, side),
        out_shape=(
            jax.ShapeDtypeStruct((tok_dev, HD), F32),
            jax.ShapeDtypeStruct((tok_dev, HD), F32),
            jax.ShapeDtypeStruct((2, 4, tok_dev, HD), BF16),
        ),
        in_specs=[smem, vmem, vmem, vmem],
        out_specs=(vmem, vmem, vmem),
    )(block_pairs, freq, keys, values)
    held = [
        pltpu.VMEM((2, signs(h, far) * side, 4, tok_dev, HD), BF16) for h in range(far + 1)
    ]
    got = [pltpu.SemaphoreType.DMA((signs(h, far) * side,)) for h in range(far + 1)]
    mixture, weight, picked = pl.pallas_call(
        functools.partial(attend, side),
        out_shape=(
            jax.ShapeDtypeStruct((KVH, 2 * HD, rows), F32),
            jax.ShapeDtypeStruct((KVH, 2, 8, rows), F32),
            jax.ShapeDtypeStruct((4, devices, HD), F32),
        ),
        in_specs=[smem, smem, vmem, pl.BlockSpec(memory_space=pl.ANY), vmem, vmem],
        out_specs=(vmem, vmem, vmem),
        scratch_shapes=[
            *held,
            *held,
            *got,
            *got,
            pltpu.VMEM((tok_dev, QH * HD), BF16),
            pltpu.VMEM((KVH, rows, 2 * HD), BF16),
            pltpu.VMEM((KVH, 2, 1, rows), F32),
            pltpu.VMEM((KVH, 2, 8, rows), F32),
            pltpu.VMEM((2, 4, devices, HD), F32),
            pltpu.SemaphoreType.DMA,
            pltpu.SemaphoreType.DMA((2,)),
            pltpu.SemaphoreType.DMA((2,)),
            pltpu.SemaphoreType.DMA((2, far)),
            pltpu.SemaphoreType.DMA((2, far + 1)),
            pltpu.SemaphoreType.DMA((2, far + 1)),
        ],
        compiler_params=pltpu.CompilerParams(
            collective_id=0, has_side_effects=True, vmem_limit_bytes=60 * 1024 * 1024
        ),
    )(block_pairs, decode_slots, packed, queries, cosine, sine)
    attended, cache = pl.pallas_call(
        functools.partial(finish, side),
        out_shape=(
            jax.ShapeDtypeStruct((tok_dev, QH * HD), BF16),
            jax.ShapeDtypeStruct((2 * devices, 2 * HD), BF16),
        ),
        in_specs=[smem, vmem, vmem, vmem, vmem],
        out_specs=(vmem, vmem),
    )(decode_slots, block_pairs[None, :], mixture, weight, picked)
    return attended, cache.reshape(1, 2 * devices, 2, HD)


def solution(mesh):
    side = math.isqrt(mesh.shape["seq"] // 2)
    placed = (
        P(("groups", "seq"), None),
        P(("groups", "seq"), None),
        P(("groups", "seq"), None),
        P("groups"),
        P("groups"),
    )
    return jax.shard_map(
        functools.partial(shards, side),
        mesh=mesh,
        in_specs=placed,
        out_specs=(P(("groups", "seq"), None), P(("groups", "seq"), None, None, None)),
        check_vma=False,
    )
```
